256 devices in a mesh: section: 16 (over y, x_hi, core), ctx: 16 (over z, x_lo).
Axes of the slice: x: 4 (x_hi: 2, x_lo: 2; x = x_hi * 2 + x_lo), y: 4, z: 8, core: 2. Of those that a mesh axis runs over, the one named last changes fastest.
Arguments:
- section_inputs: bfloat16 [16, 1792, 2048], P('section', 'ctx'), may hold values from -3 to 3
- saved_inputs: bfloat16 [16, 1792, 2048], P('section', 'ctx'), may hold values from -3 to 3
- output_grads: bfloat16 [16, 1792, 2048], P('section', 'ctx'), may hold values from -6 to 6
- token_positions: int32 [1792], P('ctx'), may hold values from 0 to 1791, each once
- norm_gain: float32 [16, 2048], P('section'), may hold values from 0.7 to 6
- query_weight: bfloat16 [16, 2048, 2048], P('section', 'ctx'), may hold values from -0.13258252 to 0.13258252
- keyval_weight: bfloat16 [16, 2048, 1024], P('section', 'ctx'), may hold values from -0.13258252 to 0.13258252
- output_weight: bfloat16 [16, 2048, 2048], P('section'), may hold values from -0.125 to 0.125
Outputs:
- next_inputs: bfloat16 [16, 1792, 2048], P('section', 'ctx')
- input_grads: bfloat16 [16, 1792, 2048], P('section', 'ctx')
The draws below stay inside these ranges and needn't reach their ends.
Inputs may be any that keep to these rules, and one draw needn't show every extreme that they name: `token_positions`: each position of the sequence once.
All inputs are finite; a program needn't handle non-finite values.
Results may differ from the reference program's by a relative error of at most 0.04.
The reference program's roundings to bfloat16 on the way (of `normed`, `rounded` and `mixed`) count: a program that leaves them out, or rounds other values in their place, can miss the bound.
Values may be sent and summed in bfloat16 or wider, within the bound.
No kernel may reach another device: no remote copies, remote signals or barrier semaphores. Data moves between devices by JAX's collectives and lax.ppermute only.
A program may use at most 192 MiB of HBM per device.

```python
import jax
import jax.numpy as jnp
from jax import lax

D = 2048
HEADS = 16
KV_HEADS = 4
HEAD_DIM = 128
SECTIONS = 16
SEQ = 1792


def paired_weights(key):
    query_key = jax.random.fold_in(key, 11)
    keyval_key = jax.random.fold_in(key, 12)
    query_matrix = jax.random.truncated_normal(query_key, -4.0, 4.0, (SECTIONS, D, HEADS * HEAD_DIM), jnp.float32) * D ** (-0.5)
    keyval_matrix = jax.random.truncated_normal(keyval_key, -4.0, 4.0, (SECTIONS, D, 2 * KV_HEADS * HEAD_DIM), jnp.float32) * D ** (-0.5)
    return (query_matrix, keyval_matrix)


def draw_query_weight(key, part):
    return paired_weights(key)[0].astype(jnp.bfloat16)


def draw_keyval_weight(key, part):
    return paired_weights(key)[1].astype(jnp.bfloat16)


def draw_norm_gain(key, part):
    gain_key = jax.random.fold_in(key, 21)
    return 1.0 + 0.1 * jax.random.truncated_normal(gain_key, -3.0, 3.0, (SECTIONS, D), jnp.float32)


def block_levels(key, dims, shards, low, top_value):
    level, own = 1.0, jax.random.fold_in(key, 6)
    for axis_at, shards_of in shards:
        steps = jnp.exp(jax.random.uniform(jax.random.fold_in(own, axis_at), (shards_of,), jnp.float32, low / len(shards), top_value / len(shards)))
        level = level * jnp.repeat(steps, dims[axis_at] // shards_of).reshape([-1 if axis == axis_at else 1 for axis in range(len(dims))])
    return level


def normal_values(key, shape, spread, bound, cuts=(), kind=jnp.bfloat16):
    array = spread * jax.random.normal(key, shape, jnp.float32)
    if cuts:
        array = array * block_levels(key, shape, cuts, -0.22, 0.18)
    return jnp.clip(array, -bound, bound).astype(kind)


def setup_inputs(seed: int = 0) -> dict:
    keys = jax.random.split(jax.random.key(seed), 9)
    section_inputs = normal_values(keys[0], (SECTIONS, SEQ, D), 0.5, 3.0, ((0, 16), (1, 16)))
    saved_inputs = normal_values(keys[1], (SECTIONS, SEQ, D), 0.5, 3.0, ((0, 16), (1, 16)))
    output_grads = normal_values(keys[2], (SECTIONS, SEQ, D), 1.0, 6.0, ((0, 16), (1, 16)))
    token_positions = jax.random.permutation(keys[3], SEQ).astype(jnp.int32)
    norm_gain = draw_norm_gain(jax.random.fold_in(keys[8], 71), 0)
    query_weight = draw_query_weight(jax.random.fold_in(keys[8], 71), 0)
    keyval_weight = draw_keyval_weight(jax.random.fold_in(keys[8], 71), 0)
    output_weight = normal_values(keys[7], (SECTIONS, HEADS * HEAD_DIM, D), (HEADS * HEAD_DIM) ** -0.5, 0.125, ((0, 16),))
    return {"section_inputs": section_inputs, "saved_inputs": saved_inputs, "output_grads": output_grads, "token_positions": token_positions, "norm_gain": norm_gain, "query_weight": query_weight, "keyval_weight": keyval_weight, "output_weight": output_weight}


norm_eps = 1e-05
rope_base = 500000.0

def rotate(matrix, positions):
    half_dim = matrix.shape[-1] // 2
    frequency = rope_base ** (-2.0 * jnp.arange(half_dim, dtype=jnp.float32) / matrix.shape[-1])
    angles = positions.astype(jnp.float32)[:, None] * frequency[None, :]
    cos_table = jnp.cos(angles)[:, None, :]
    sin_table = jnp.sin(angles)[:, None, :]
    leading = matrix[..., :half_dim]
    trailing = matrix[..., half_dim:]
    return jnp.concatenate([leading * cos_table - trailing * sin_table, trailing * cos_table + leading * sin_table], axis=-1)

def project(tokens, gain, query_matrix, keyval_matrix, positions):
    widened = tokens.astype(jnp.float32)
    inverse = lax.rsqrt(lax.optimization_barrier(jnp.mean(widened * widened, axis=-1, keepdims=True)) + norm_eps)
    normed = (widened * inverse * gain[None, :]).astype(jnp.bfloat16)
    row_count = tokens.shape[0]
    query_full = jnp.dot(normed, query_matrix, preferred_element_type=jnp.float32)
    keyval_full = jnp.dot(normed, keyval_matrix, preferred_element_type=jnp.float32)
    queries = rotate(query_full.reshape(row_count, -1, HEAD_DIM), positions).astype(jnp.bfloat16)
    paired = keyval_full.reshape(row_count, 2, -1, HEAD_DIM)
    key_rows = rotate(paired[:, 0], positions).astype(jnp.bfloat16)
    value_rows = paired[:, 1].astype(jnp.bfloat16)
    return (queries, key_rows, value_rows)

def attend(queries, key_wide, value_wide, query_pos, key_pos):
    row_count = queries.shape[0]
    group_size = queries.shape[1] // key_wide.shape[1]
    grouped = queries.astype(jnp.float32).reshape(row_count, key_wide.shape[1], group_size, queries.shape[2])
    scores = jnp.einsum('rkgd,skd->kgrs', grouped, key_wide) * queries.shape[2] ** (-0.5)
    visible = (key_pos[None, :] <= query_pos[:, None])[None, None]
    masked = jnp.where(visible, scores, -1e+30)
    row_max = lax.stop_gradient(lax.optimization_barrier(jnp.max(masked, axis=-1, keepdims=True)))
    numerators = jnp.where(visible, jnp.exp(masked - row_max), 0.0)
    totals = lax.optimization_barrier(jnp.sum(numerators, axis=-1))
    rounded = lax.optimization_barrier(numerators.astype(jnp.bfloat16)).astype(jnp.float32)
    summed = jnp.einsum('kgrs,skd->rkgd', rounded, value_wide)
    averaged = summed / jnp.transpose(totals, (2, 0, 1))[..., None]
    return averaged.reshape(row_count, -1).astype(jnp.bfloat16)

def finish(tokens, mixed, output_matrix):
    return (tokens.astype(jnp.float32) + jnp.dot(mixed, output_matrix, preferred_element_type=jnp.float32)).astype(jnp.bfloat16)

def section_layer(tokens, gain, query_matrix, keyval_matrix, output_matrix, positions):
    queries, key_rows, value_rows = project(tokens, gain, query_matrix, keyval_matrix, positions)
    mixed = attend(queries, key_rows.astype(jnp.float32), value_rows.astype(jnp.float32), positions, positions)
    return finish(tokens, mixed, output_matrix)

def reference(section_inputs, saved_inputs, output_grads, token_positions, norm_gain, query_weight, keyval_weight, output_weight):

    def one_section(packed):
        forward_tokens, saved_tokens, upstream, gain, query_matrix, keyval_matrix, output_matrix = packed

        def layer(tokens):
            return section_layer(tokens, gain, query_matrix, keyval_matrix, output_matrix, token_positions)
        produced = layer(forward_tokens)
        unused, back_layer = jax.vjp(layer, saved_tokens)
        token_grads, = back_layer(upstream)
        return (produced, token_grads)
    results, gradients = lax.map(one_section, (section_inputs, saved_inputs, output_grads, norm_gain, query_weight, keyval_weight, output_weight))
    return (jnp.roll(results, 1, axis=0), jnp.roll(gradients, -1, axis=0))
```

```python
import functools

import jax
import jax.numpy as jnp
from jax import lax
from jax.experimental import pallas as pl
from jax.experimental.pallas import tpu as pltpu
from jax.sharding import Mesh
from jax.sharding import PartitionSpec as P

HEAD_DIM = 128
GROUP = 4
Z = 8
X = 2
OFFSETS = (0, -1, -2, -3, 1, 2, 3, 4)

norm_eps = 1e-05
rope_base = 500000.0


def shift(block, axis, distance):
    n = lax.axis_size(axis)
    return lax.ppermute(block, axis, [(i, (i + distance) % n) for i in range(n)])


def ring_gather(block):
    up, down = [block], [block]
    for _ in range(3):
        up.append(shift(up[-1], "z", 1))
        down.append(shift(down[-1], "z", -1))
    half = block.shape[0] // 2
    far = jnp.concatenate([shift(up[-1][:half], "z", 1), shift(down[-1][half:], "z", -1)], axis=0)
    return up + down[1:] + [far]


def f32(v):
    return v.astype(jnp.float32)


def bf16(v):
    return v.astype(jnp.bfloat16)


def ring_scatter(parts):
    at = dict(zip(OFFSETS, parts))
    high, low = at[4], at[-3]
    for k in (3, 2, 1, 0):
        high = f32(shift(high, "z", 1)) + f32(at[k])
        high = bf16(high) if k else high
    for k in (-2, -1):
        low = bf16(f32(shift(low, "z", -1)) + f32(at[k]))
    return bf16(high + f32(shift(low, "z", -1)))


def order_by_ring(array, z, x, axis):
    array = jnp.where(x == 0, array, jnp.flip(array, axis + 1))
    twice = jnp.concatenate([array, array], axis=axis)
    near = lax.dynamic_slice_in_dim(twice, z, Z, axis)
    pieces = [lax.slice_in_dim(near, o % Z, o % Z + 1, axis=axis) for o in OFFSETS]
    return jnp.concatenate(pieces, axis=axis)


def order_back(array, z, x, axis):
    at = {o % Z: i for i, o in enumerate(OFFSETS)}
    pieces = [lax.slice_in_dim(array, at[r], at[r] + 1, axis=axis) for r in range(Z)]
    twice = jnp.concatenate(pieces + pieces, axis=axis)
    array = lax.dynamic_slice_in_dim(twice, Z - z, Z, axis)
    return jnp.where(x == 0, array, jnp.flip(array, axis + 1))


def turn(block, cos_table, sin_table):
    return block * cos_table + pltpu.roll(block, HEAD_DIM // 2, 1) * sin_table


def stacked_heads(ref, change=lambda v: v):
    return jnp.concatenate(
        [change(ref[:, HEAD_DIM * j : HEAD_DIM * (j + 1)]) for j in range(GROUP)], axis=0
    )


def unstacked(rows, ref, change=lambda v: v):
    count = rows.shape[0] // GROUP
    for j in range(GROUP):
        ref[:, HEAD_DIM * j : HEAD_DIM * (j + 1)] = change(rows[count * j : count * (j + 1)])


def dot(a, b, dims):
    return lax.dot_general(a, b, (dims, ((), ())), preferred_element_type=jnp.float32)


def softmax_parts(queries, keys, query_pos, key_pos):
    scores = dot(keys, queries, ((1,), (1,))) * HEAD_DIM ** (-0.5)
    masked = jnp.where(key_pos <= query_pos, scores, -1e30)
    numerators = jnp.exp(masked - jnp.max(masked, axis=0, keepdims=True))
    return numerators, jnp.sum(numerators, axis=0, keepdims=True)


def forward_body(q_ref, k_ref, v_ref, qp_ref, kp_ref, c_ref, s_ref, o_ref):
    rotated = lambda v: bf16(turn(v, c_ref[...], s_ref[...]))
    queries = stacked_heads(q_ref, rotated)
    numerators, totals = softmax_parts(queries, k_ref[...], qp_ref[...], kp_ref[...])
    averaged = dot(v_ref[...], bf16(numerators), ((0,), (0,))) / totals
    unstacked(bf16(averaged.T), o_ref)


def backward_body(
    q_ref, k_ref, v_ref, g_ref, qp_ref, kp_ref, c_ref, s_ref, dq_ref, dk_ref, dv_ref
):
    rotated = lambda v: bf16(turn(v, c_ref[...], s_ref[...]))
    back = lambda v: bf16(turn(f32(bf16(v)), c_ref[...], -s_ref[...]))
    queries = stacked_heads(q_ref, rotated)
    keys, values = k_ref[...], v_ref[...]
    grads = stacked_heads(g_ref)
    numerators, totals = softmax_parts(queries, keys, qp_ref[...], kp_ref[...])
    rounded = bf16(numerators)
    averaged = dot(values, rounded, ((0,), (0,))) / totals
    grads_t = f32(grads).T
    level = jnp.sum(grads_t * averaged, axis=0, keepdims=True)
    dv_ref[...] = bf16(dot(rounded, bf16(grads_t / totals), ((1,), (1,))))
    pulled = dot(values, grads, ((1,), (1,)))
    scores_grad = bf16(numerators * (pulled - level) * (HEAD_DIM ** (-0.5) / totals))
    dk_ref[...] = bf16(dot(scores_grad, queries, ((1,), (0,))))
    unstacked(dot(keys, scores_grad, ((0,), (0,))).T, dq_ref, back)


def attention_specs(rows, count):
    wide = pl.BlockSpec((rows, GROUP * HEAD_DIM), lambda h: (0, h))
    key = pl.BlockSpec((count, HEAD_DIM), lambda h: (0, h))
    value = pl.BlockSpec((count, HEAD_DIM), lambda h: (0, h + 2))
    whole = [
        pl.BlockSpec((1, GROUP * rows), lambda h: (0, 0)),
        pl.BlockSpec((count, 1), lambda h: (0, 0)),
        pl.BlockSpec((rows, HEAD_DIM), lambda h: (0, 0)),
        pl.BlockSpec((rows, HEAD_DIM), lambda h: (0, 0)),
    ]
    return wide, key, value, whole


def attend(queries, keyvals, tables):
    rows, count = queries.shape[0], keyvals.shape[0]
    wide, key, value, whole = attention_specs(rows, count)
    flops = 2 * 2 * 8 * rows * count * HEAD_DIM
    return pl.pallas_call(
        forward_body,
        grid=(2,),
        in_specs=[wide, key, value, *whole],
        out_specs=wide,
        out_shape=jax.ShapeDtypeStruct((rows, 8 * HEAD_DIM), jnp.bfloat16),
        cost_estimate=pl.CostEstimate(flops=flops, bytes_accessed=4 << 20, transcendentals=0),
        compiler_params=pltpu.CompilerParams(vmem_limit_bytes=56 << 20),
        name="attend",
    )(queries, keyvals, keyvals, *tables)


def attend_back(queries, keyvals, grads, tables):
    rows, count = queries.shape[0], keyvals.shape[0]
    wide, key, value, whole = attention_specs(rows, count)
    flops = 6 * 2 * 8 * rows * count * HEAD_DIM
    return pl.pallas_call(
        backward_body,
        grid=(2,),
        in_specs=[wide, key, value, wide, *whole],
        out_specs=[wide, key, key],
        out_shape=[
            jax.ShapeDtypeStruct((rows, 8 * HEAD_DIM), jnp.bfloat16),
            jax.ShapeDtypeStruct((count, 2 * HEAD_DIM), jnp.bfloat16),
            jax.ShapeDtypeStruct((count, 2 * HEAD_DIM), jnp.bfloat16),
        ],
        cost_estimate=pl.CostEstimate(flops=flops, bytes_accessed=6 << 20, transcendentals=0),
        compiler_params=pltpu.CompilerParams(vmem_limit_bytes=56 << 20),
        name="attend_back",
    )(queries, keyvals, keyvals, grads, *tables)


def turn_heads(matrix, cos_table, sin_table):
    heads = matrix.reshape(matrix.shape[0], -1, HEAD_DIM)
    half = HEAD_DIM // 2
    swapped = jnp.concatenate([heads[..., half:], heads[..., :half]], axis=-1)
    return (heads * cos_table[:, None, :] + swapped * sin_table[:, None, :]).reshape(matrix.shape)


def halves(array, x):
    width = array.shape[1] // 2
    own = lax.dynamic_slice_in_dim(array, x * width, width, 1)
    other = lax.dynamic_slice_in_dim(array, (1 - x) * width, width, 1)
    return own, other


def shards(
    section_inputs,
    saved_inputs,
    output_grads,
    token_positions,
    norm_gain,
    query_weight,
    keyval_weight,
    output_weight,
):
    z, x = lax.axis_index("z"), lax.axis_index("x")
    swap = lambda v: shift(v, "x", 1)
    gain = norm_gain[0]
    tokens, saved, upstream = section_inputs[0], saved_inputs[0], output_grads[0]
    wo = output_weight[0]
    count = tokens.shape[0]
    rows = X * count

    wk_own, wk_other = halves(keyval_weight[0][:, :512], x)
    wv_own, wv_other = halves(keyval_weight[0][:, 512:], x)
    wq_own, wq_other = halves(query_weight[0], x)
    wkv_shard = jnp.concatenate(
        [
            jnp.concatenate([wk_own, wv_own], axis=1),
            swap(jnp.concatenate([wk_other, wv_other], axis=1)),
        ],
        axis=0,
    )
    wkv = jnp.concatenate(ring_gather(wkv_shard), axis=0)
    wq_shard = jnp.concatenate([wq_own, swap(wq_other)], axis=0)
    wq = jnp.concatenate(ring_gather(wq_shard), axis=0)

    spread = lax.all_gather(token_positions, ("z", "x"), axis=0, tiled=True)
    key_pos = order_by_ring(spread.reshape(Z, X, count), z, x, 0).reshape(-1)
    query_pos = key_pos[:rows]
    frequency = rope_base ** (
        -2.0 * jnp.arange(HEAD_DIM // 2, dtype=jnp.float32) / HEAD_DIM
    )
    angles = f32(query_pos)[:, None] * frequency[None, :]
    cos_half, sin_half = jnp.cos(angles), jnp.sin(angles)
    cos_table = jnp.concatenate([cos_half, cos_half], axis=1)
    sin_table = jnp.concatenate([-sin_half, sin_half], axis=1)
    tables = (
        jnp.tile(query_pos, GROUP)[None, :],
        key_pos[:, None],
        cos_table,
        sin_table,
    )

    def scaled(block):
        wide = f32(block)
        inverse = lax.rsqrt(jnp.mean(wide * wide, axis=-1, keepdims=True) + norm_eps)
        return bf16(wide * inverse * gain[None, :]), inverse

    normed_saved, inverse_saved = scaled(saved)
    normed_tokens, _ = scaled(tokens)
    normed = jnp.concatenate(
        [normed_saved, swap(normed_saved), normed_tokens, swap(normed_tokens)], axis=0
    )
    normed = order_by_ring(normed.reshape(2 * rows, Z, X, HEAD_DIM), z, x, 1)
    normed = normed.reshape(2 * rows, -1)

    mixed_grad = bf16(dot(upstream, wo, ((1,), (1,))))
    mg_own, mg_other = halves(mixed_grad, x)
    mixed_grads = jnp.concatenate([mg_own, swap(mg_other)], axis=0)

    both = dot(normed, wkv, ((1,), (0,)))
    turned = turn_heads(
        both[:, :256], jnp.tile(cos_table, (2, 1)), jnp.tile(sin_table, (2, 1))
    )
    keyvals = jnp.concatenate([bf16(turned), bf16(both[:, 256:])], axis=1)
    kv_saved = jnp.concatenate(ring_gather(keyvals[:rows]), axis=0)
    kv_tokens = jnp.concatenate(ring_gather(keyvals[rows:]), axis=0)
    queries = dot(normed, wq, ((1,), (0,)))

    dq, dk, dv = attend_back(queries[:rows], kv_saved, mixed_grads, tables)
    dkv = jnp.concatenate([dk, dv], axis=1)
    dkv = ring_scatter([dkv[rows * i : rows * (i + 1)] for i in range(Z)])

    mixed = attend(queries[rows:], kv_tokens, tables)
    received = swap(mixed[count:])
    mixed = jnp.where(
        x == 0,
        jnp.concatenate([mixed[:count], received], axis=1),
        jnp.concatenate([received, mixed[:count]], axis=1),
    )
    produced = bf16(f32(tokens) + dot(mixed, wo, ((1,), (0,))))
    sent_on = shift(produced, "section", 1)

    dk_full = bf16(turn_heads(f32(dkv[:, :256]), cos_table, -sin_table))
    dkv_full = jnp.concatenate([dk_full, dkv[:, 256:]], axis=1)
    dnormed = bf16(dot(dq, wq, ((1,), (1,))) + dot(dkv_full, wkv, ((1,), (1,))))
    received = jnp.flip(swap(dnormed[count:]).reshape(count, Z, X, HEAD_DIM), 2)
    dnormed = bf16(f32(dnormed[:count].reshape(count, Z, X, HEAD_DIM)) + f32(received))
    dnormed = f32(order_back(dnormed, z, x, 1).reshape(count, -1)) * gain[None, :]
    wide = f32(saved)
    share = jnp.mean(dnormed * wide, axis=-1, keepdims=True) * inverse_saved**3
    project_grad = bf16(dnormed * inverse_saved - wide * share)
    sent_back = shift(upstream + project_grad, "section", -1)
    return (sent_on[None], sent_back[None])


def solution(mesh):
    sections = mesh.shape["section"]
    torus = Mesh(mesh.devices.reshape(sections, Z, X), ("section", "z", "x"))
    ctx = ("z", "x")
    placed = (
        P("section", ctx, None),
        P("section", ctx, None),
        P("section", ctx, None),
        P(ctx),
        P("section", None),
        P("section", ctx, None),
        P("section", ctx, None),
        P("section", None, None),
    )
    return jax.shard_map(
        shards,
        mesh=torus,
        in_specs=placed,
        out_specs=(P("section", ctx, None), P("section", ctx, None)),
        check_vma=False,
    )
```
